32 devices in a mesh: replica: 2 (over x), batch: 16 (over z, y, core).
Axes of the slice: x: 2, y: 2, z: 4, core: 2. Of those that a mesh axis runs over, the one named last changes fastest.
Arguments:
- cache_state: bfloat16 [256, 12, 64, 128], P(('replica', 'batch')), parts along dimension 0, may hold values from -6 to 6
- prefill_state: bfloat16 [64, 12, 64, 128], P(('replica', 'batch')), parts along dimension 0, may hold values from -6 to 6
- x_in: bfloat16 [256, 768], P(('replica', 'batch')), parts along dimension 0, may hold values from -6 to 6
- z_in: bfloat16 [256, 768], P(('replica', 'batch')), parts along dimension 0, may hold values from -6 to 6
- b_in: bfloat16 [256, 128], P(('replica', 'batch')), parts along dimension 0, may hold values from -6 to 6
- c_in: bfloat16 [256, 128], P(('replica', 'batch')), parts along dimension 0, may hold values from -0.59765625 to 0.59765625
- dt_in: bfloat16 [256, 12], P(('replica', 'batch')), parts along dimension 0, may hold values from -4 to 4
- dt_bias: float32 [12], replicated, may hold values from -3 to 0.5
- a_log: float32 [12], replicated, may hold values from 0 to 2.5
- d_skip: float32 [12], replicated, may hold values from 0.5 to 1.5
- norm_gain: float32 [768], replicated, may hold values from 0.25 to 1.75
- out_weight: bfloat16 [768, 4096], replicated, may hold values from -0.21875 to 0.21875
- active: int32 [256], P(('replica', 'batch')), parts along dimension 0, may hold values from 0 to 1, as said below
- prefill_count: int32 [32], P(('replica', 'batch')), parts along dimension 0, may hold values from 0 to 2, as said below
- dest_owner: int32 [64], P(('replica', 'batch')), parts along dimension 0, may hold values from 0 to 15, as said below
- dest_slot: int32 [64], P(('replica', 'batch')), parts along dimension 0, may hold values from 0 to 7, as said below
Outputs:
- mixed: bfloat16 [256, 4096], P(('replica', 'batch')), parts along dimension 0
- new_state: bfloat16 [256, 12, 64, 128], P(('replica', 'batch')), parts along dimension 0
The draws below stay inside these ranges and needn't reach their ends.
There are 2 independent parts, one for each index of `replica`. The reference program is written for one: setup_inputs(seed, part) draws one part's arguments, and reference() takes and returns one part's arrays. A program takes and returns all parts, laid end to end along the dimension named above; an argument that names none is the same for every part. Nothing has to cross between parts.
Inputs may be any that keep to these rules, and one draw needn't show every extreme that they name: `active`: at least 2 slots of every device are 0. `prefill_count`: the live rows of a device are its first ones. `dest_owner`: for each row index j below 2, the rows j of the devices go to distinct owners; the two rows of one device go to different owners. So an owner receives at most 2 live rows, at most one from any device, and some owner exactly 2. `dest_slot`: A live row's slot is 0 in the owner's active entries, and no two live rows share an owner and slot.
All inputs are finite; a program needn't handle non-finite values.
Results may differ from the reference program's by a relative error of at most 0.0049.
Values may be sent and summed in bfloat16 or wider, within the bound.
A program may use at most 128 MiB of HBM per device.

```python
import jax
import jax.numpy as jnp
from jax import lax

DM = 4096
HEADS = 12
HEAD_DIM = 64
STATE = 128
SLOTS = 8
P_DEV = 2
ROWS = 128
NEW = 32
INNER = 768
N_BATCH = 16


def migration_plan(key):
    base = jax.random.fold_in(key, 7)
    k_perm, k_center, k_count, k_order, k_active, k_offset = jax.random.split(base, 6)
    device_ids = jnp.arange(N_BATCH, dtype=jnp.int32)
    first = jax.random.permutation(k_perm, N_BATCH).astype(jnp.int32)
    center = jax.random.randint(k_center, (), 0, N_BATCH).astype(jnp.int32)
    far_owner = ((center + N_BATCH // 2) % N_BATCH).astype(jnp.int32)
    where_far = jnp.argmax((first == far_owner).astype(jnp.int32)).astype(jnp.int32)
    former = first[center]
    first = first.at[where_far].set(former)
    first = first.at[center].set(far_owner)
    offset = jax.random.randint(k_offset, (), 1, N_BATCH).astype(jnp.int32)
    second = first[(device_ids + offset) % N_BATCH]
    owners = jnp.stack([first, second], axis=1).astype(jnp.int32)
    counts = jax.random.randint(k_count, (N_BATCH,), 0, P_DEV + 1)
    full = (device_ids == center) | (device_ids == (center - offset) % N_BATCH)
    counts = jnp.where(full, P_DEV, counts).astype(jnp.int32)
    scores = jax.random.randint(k_order, (N_BATCH, SLOTS), 0, 1 << 20) * SLOTS + jnp.arange(SLOTS, dtype=jnp.int32)[None, :]
    order = jnp.argsort(scores, axis=1).astype(jnp.int32)
    reserved = order[:, :P_DEV]
    column = jnp.broadcast_to(jnp.arange(P_DEV, dtype=jnp.int32)[None, :], (N_BATCH, P_DEV))
    slots = reserved[owners, column].astype(jnp.int32)
    held = jnp.any(reserved[:, :, None] == jnp.arange(SLOTS, dtype=jnp.int32)[None, None, :], axis=1)
    running = jax.random.randint(k_active, (N_BATCH, SLOTS), 0, 4) > 0
    active = jnp.where(held, 0, running.astype(jnp.int32)).astype(jnp.int32)
    return (active.reshape(-1), counts, owners.reshape(-1), slots.reshape(-1))


def draw_active(key, part):
    return migration_plan(key)[0]


def draw_prefill_count(key, part):
    return migration_plan(key)[1]


def draw_dest_owner(key, part):
    return migration_plan(key)[2]


def draw_dest_slot(key, part):
    return migration_plan(key)[3]


def block_levels(key, dims, pieces, least, high):
    loudness = 1.0
    for position, parts in pieces:
        draws = jax.random.uniform(jax.random.fold_in(jax.random.fold_in(key, 6), position), (parts,), jnp.float32, least / len(pieces), high / len(pieces))
        loudness = loudness * jnp.repeat(jnp.exp(draws), dims[position] // parts).reshape((-1,) + (1,) * (len(dims) - 1 - position))
    return loudness


def gaussian(key, shape, spread, most, cuts=(), kind=jnp.bfloat16):
    loudness = block_levels(key, shape, cuts, -0.22, 0.18) if cuts else 1.0
    result = jax.random.normal(key, shape, jnp.float32) * spread * loudness
    return jnp.minimum(jnp.maximum(result, -most), most).astype(kind)


def setup_inputs(seed: int = 0, part: int = 0) -> dict:
    key_of = jax.random.split(jax.random.key(seed), 17)
    part_splits = jax.random.split(jax.random.fold_in(key_of[16], part), 17)
    return {
        "cache_state": gaussian(part_splits[0], (ROWS, HEADS, HEAD_DIM, STATE), 1.0, 6.0, ((0, 16),)),
        "prefill_state": gaussian(part_splits[1], (NEW, HEADS, HEAD_DIM, STATE), 1.0, 6.0, ((0, 16),)),
        "x_in": gaussian(part_splits[2], (ROWS, INNER), 1.0, 6.0, ((0, 16),)),
        "z_in": gaussian(part_splits[3], (ROWS, INNER), 1.0, 6.0, ((0, 16),)),
        "b_in": gaussian(part_splits[4], (ROWS, STATE), 1.0, 6.0, ((0, 16),)),
        "c_in": gaussian(part_splits[5], (ROWS, STATE), 0.1, 0.59765625, ((0, 16),)),
        "dt_in": gaussian(part_splits[6], (ROWS, HEADS), 1.0, 4.0, ((0, 16),)),
        "dt_bias": jnp.clip(jax.random.uniform(key_of[7], (HEADS,), jnp.float32, -3.0, 0.5), -3.0, 0.5),
        "a_log": jnp.clip(jax.random.uniform(key_of[8], (HEADS,), jnp.float32, 0.0, 2.5), 0.0, 2.5),
        "d_skip": jnp.clip(jax.random.uniform(key_of[9], (HEADS,), jnp.float32, 0.5, 1.5), 0.5, 1.5),
        "norm_gain": jnp.clip(1.0 + 0.15 * jax.random.normal(key_of[10], (INNER,), jnp.float32), 0.25, 1.75),
        "out_weight": gaussian(key_of[11], (INNER, DM), INNER ** -0.5, 0.21875),
        "active": draw_active(jax.random.fold_in(jax.random.fold_in(key_of[16], part), 71), part),
        "prefill_count": draw_prefill_count(jax.random.fold_in(jax.random.fold_in(key_of[16], part), 71), part),
        "dest_owner": draw_dest_owner(jax.random.fold_in(jax.random.fold_in(key_of[16], part), 71), part),
        "dest_slot": draw_dest_slot(jax.random.fold_in(jax.random.fold_in(key_of[16], part), 71), part),
    }


def advance(state, x_in, z_in, b_in, c_in, dt_in, dt_bias, a_log, d_skip, norm_gain, out_weight, live):
    rows, heads, hdim, nstate = state.shape
    step = jax.nn.softplus(dt_in.astype(jnp.float32) + dt_bias[None, :])
    decay = jnp.exp(-step * jnp.exp(a_log)[None, :])
    inputs = x_in.astype(jnp.float32).reshape(rows, heads, hdim)
    b_vals = b_in.astype(jnp.float32)
    c_vals = c_in.astype(jnp.float32)
    fresh = state * decay[:, :, None, None] + (step[:, :, None] * inputs)[:, :, :, None] * b_vals[:, None, None, :]
    ys = jnp.einsum('rhpn,rn->rhp', fresh, c_vals, precision=lax.Precision.HIGHEST) + d_skip[None, :, None] * inputs
    gated = ys.reshape(rows, heads * hdim) * jax.nn.silu(z_in.astype(jnp.float32))
    scale = lax.rsqrt(lax.optimization_barrier(jnp.mean(gated * gated, axis=1, keepdims=True)) + 1e-05)
    normed = jnp.where(live[:, None], gated * scale * norm_gain[None, :], 0.0).astype(jnp.bfloat16)
    mixed = jnp.dot(normed, out_weight, preferred_element_type=jnp.float32).astype(jnp.bfloat16)
    new_state = jnp.where(live[:, None, None, None], fresh, 0.0).astype(jnp.bfloat16)
    return (mixed, new_state)

def reference(cache_state, prefill_state, x_in, z_in, b_in, c_in, dt_in, dt_bias, a_log, d_skip, norm_gain, out_weight, active, prefill_count, dest_owner, dest_slot):
    rows_all = N_BATCH * SLOTS
    source = jnp.arange(N_BATCH * P_DEV, dtype=jnp.int32)
    valid = source % P_DEV < prefill_count[source // P_DEV]
    target = jnp.where(valid, dest_owner * SLOTS + dest_slot, rows_all).astype(jnp.int32)
    state = cache_state.astype(jnp.float32).at[target].set(prefill_state.astype(jnp.float32), mode='drop')
    arrived = jnp.zeros((rows_all,), jnp.int32).at[target].set(1, mode='drop')
    live = (active > 0) | (arrived > 0)
    return advance(state, x_in, z_in, b_in, c_in, dt_in, dt_bias, a_log, d_skip, norm_gain, out_weight, live)
```

```python
import functools

import jax
import jax.numpy as jnp
from jax import lax
from jax.experimental import pallas as pl
from jax.experimental.pallas import tpu as pltpu
from jax.sharding import PartitionSpec as P

MESH = pl.DeviceIdType.MESH
ROOM = 24 * 1024 * 1024


def gather_kernel(
    n, meta_ref, pre_ref, moved_ref, info_ref, buf, meta_buf, meta_smem,
    recv_sem, left_sem, right_sem, across_sem, mate_sem, local_sem,
):
    depth = n // 4
    rows = pre_ref.shape[0]
    me = lax.axis_index("batch")
    z, y, c = me // 4, (me // 2) % 2, me % 2

    def index(zz, yy, cc):
        return (zz * 2 + yy) * 2 + cc

    left, right = index(z - 1, y, c), index(z + 1, y, c)
    across, mate = index(z, 1 - y, c), index(z, y, 1 - c)
    has_left, has_right = z > 0, z < depth - 1

    barrier = pltpu.get_barrier_semaphore()

    def greet(other):
        pl.semaphore_signal(barrier, inc=1, device_id={"batch": other}, device_id_type=MESH)

    greet(across)
    greet(mate)
    pl.when(has_left)(lambda: greet(left))
    pl.when(has_right)(lambda: greet(right))
    pl.semaphore_wait(barrier, 2 + has_left.astype(jnp.int32) + has_right.astype(jnp.int32))

    def slot(o, j):
        return meta_buf.at[o] if j == rows else buf.at[o, j]

    def mine(j):
        return meta_ref if j == rows else pre_ref.at[j]

    sent = []

    def send(cond, src, o, j, sem, target):
        copy = pltpu.make_async_remote_copy(
            src_ref=src, dst_ref=slot(o, j), send_sem=sem, recv_sem=recv_sem.at[o, j],
            device_id={"batch": target}, device_id_type=MESH,
        )
        if cond is None:
            copy.start()
        else:
            pl.when(cond)(copy.start)
        sent.append((cond, copy))

    def arrive(o, j):
        pltpu.make_async_remote_copy(
            src_ref=slot(o, j), dst_ref=slot(o, j), send_sem=local_sem.at[0],
            recv_sem=recv_sem.at[o, j], device_id={"batch": mate}, device_id_type=MESH,
        ).wait_recv()

    def both(*conds):
        return functools.reduce(jnp.logical_and, conds)

    order = (rows,) + tuple(range(rows))
    last = rows - 1
    for j in order:
        send(has_left, mine(j), me, j, left_sem.at[z, j], left)
        send(has_right, mine(j), me, j, right_sem.at[z, j], right)
    for j in (rows,) + tuple(reversed(range(rows))):
        send(None, mine(j), me, j, across_sem.at[z, j], across)
    for j in order:
        send(None, mine(j), me, j, mate_sem.at[z * 2 + y, j], mate)
    own_rows = pltpu.make_async_copy(pre_ref, buf.at[me], local_sem.at[1])
    own_meta = pltpu.make_async_copy(meta_ref, meta_buf.at[me], local_sem.at[2])
    own_rows.start()
    own_meta.start()

    def from_across(t):
        for sign in (1, -1) if t else (1,):
            zz = z + t * sign
            o = index(zz, 1 - y, c)
            inside = both(zz >= 0, zz < depth) if t else None
            for j in (rows,) + tuple(reversed(range(rows))):
                cond = inside
                if t and j == last:
                    cond = both(inside, zz > 0, zz < depth - 1)
                if cond is None:
                    arrive(o, j)
                else:
                    pl.when(cond)(functools.partial(arrive, o, j))
                if not t and j == last:
                    send(both(z == depth - 1, has_left), slot(o, j), o, j, left_sem.at[depth, j], left)
                    send(both(z == 0, has_right), slot(o, j), o, j, right_sem.at[depth, j], right)
                send(cond, slot(o, j), o, j, mate_sem.at[zz * 2 + 1 - y, j], mate)

    for s in range(1, depth):
        for j in order:
            for sign in (1, -1):
                zz = z + s * sign
                o = index(zz, y, c)
                inside = both(zz >= 0, zz < depth)
                pl.when(inside)(functools.partial(arrive, o, j))
                if sign == 1:
                    send(both(inside, has_left), slot(o, j), o, j, left_sem.at[zz, j], left)
                else:
                    send(both(inside, has_right), slot(o, j), o, j, right_sem.at[zz, j], right)
                cond = both(inside, zz > 0, zz < depth - 1) if j == last else inside
                send(cond, slot(o, j), o, j, across_sem.at[zz, j], across)
                send(inside, slot(o, j), o, j, mate_sem.at[zz * 2 + y, j], mate)
        from_across(s - 1)
    if depth > 1:
        o = index(depth - 1, 1 - y, c)
        pl.when(has_right)(functools.partial(arrive, o, last))
        send(both(has_right, has_left), slot(o, last), o, last, left_sem.at[depth, last], left)
        send(has_right, slot(o, last), o, last, mate_sem.at[(depth - 1) * 2 + 1 - y, last], mate)
        o = index(0, 1 - y, c)
        pl.when(has_left)(functools.partial(arrive, o, last))
        send(both(has_right, has_left), slot(o, last), o, last, right_sem.at[depth, last], right)
        send(has_left, slot(o, last), o, last, mate_sem.at[1 - y, last], mate)
    from_across(depth - 1)
    own_rows.wait()
    own_meta.wait()

    def of_mate(j):
        def one(k, carry):
            arrive(k * 2 + 1 - c, j)
            return carry
        lax.fori_loop(0, 2 * depth, one, 0)

    of_mate(rows)
    numbers = pltpu.make_async_copy(meta_buf, meta_smem, local_sem.at[3])
    numbers.start()
    numbers.wait()

    picks = []
    for j in range(rows):
        def look(d, carry, j=j):
            hit = meta_smem[d, 0, j] == me
            source, place = carry
            return jnp.where(hit, d, source), jnp.where(hit, meta_smem[d, 0, rows + j], place)
        source, place = lax.fori_loop(0, n, look, (jnp.int32(0), jnp.int32(-1)))
        picks.append(source)
        info_ref[j] = place
    for j in range(rows):
        of_mate(j)
    for j in range(rows):
        moved_ref[j] = buf[picks[j], j]
    for cond, copy in sent:
        if cond is None:
            copy.wait_send()
        else:
            pl.when(cond)(copy.wait_send)


def gather_rows(meta, prefill_state, n):
    rows = prefill_state.shape[0]
    depth = n // 4
    dma = pltpu.SemaphoreType.DMA
    vmem = pl.BlockSpec(memory_space=pltpu.VMEM)
    return pl.pallas_call(
        functools.partial(gather_kernel, n),
        out_shape=(
            jax.ShapeDtypeStruct(prefill_state.shape, prefill_state.dtype),
            jax.ShapeDtypeStruct((rows,), jnp.int32),
        ),
        in_specs=[vmem, vmem],
        out_specs=(vmem, pl.BlockSpec(memory_space=pltpu.SMEM)),
        scratch_shapes=[
            pltpu.VMEM((n,) + prefill_state.shape, prefill_state.dtype),
            pltpu.VMEM((n,) + meta.shape, jnp.int32),
            pltpu.SMEM((n,) + meta.shape, jnp.int32),
            dma((n, rows + 1)),
            dma((depth + 1, rows + 1)),
            dma((depth + 1, rows + 1)),
            dma((depth, rows + 1)),
            dma((2 * depth, rows + 1)),
            dma((4,)),
        ],
        compiler_params=pltpu.CompilerParams(
            collective_id=0, has_side_effects=True, vmem_limit_bytes=ROOM + 4 * 1024 * 1024
        ),
        name="gather_rows",
    )(meta, prefill_state)


def step_kernel(
    info_ref, active_ref, cache_ref, moved_ref, weight_ref, x_ref, z_ref, b_ref, c_ref, dt_ref,
    bias_ref, log_ref, skip_ref, gain_ref, mixed_ref, new_ref, states, fresh, weight,
    step_rows, decay_rows, in_sem, out_sem, weight_sem,
):
    slots, heads, hdim, nstate = cache_ref.shape
    inner = heads * hdim
    moves = moved_ref.shape[0]
    f32 = jnp.float32

    def load(r):
        hit = [info_ref[j] == r for j in range(moves)]
        held = functools.reduce(jnp.logical_or, hit)
        for j in range(moves):
            pl.when(hit[j])(
                pltpu.make_async_copy(moved_ref.at[j], states.at[r], in_sem.at[r]).start
            )
        pl.when(jnp.logical_not(held))(
            pltpu.make_async_copy(cache_ref.at[r], states.at[r], in_sem.at[r]).start
        )
        return jnp.where(jnp.logical_or(held, active_ref[r] > 0), 1.0, 0.0).astype(f32)

    live_scalars = [load(r) for r in range(slots)]
    weights = pltpu.make_async_copy(weight_ref, weight, weight_sem)
    weights.start()

    row_id = lax.broadcasted_iota(jnp.int32, (slots, 128), 0)
    live = jnp.zeros((slots, 128), f32)
    for r in range(slots):
        live = jnp.where(row_id == r, live_scalars[r], live)

    step = jax.nn.softplus(dt_ref[...].astype(f32) + bias_ref[...])
    decay = jnp.exp(-step * jnp.exp(log_ref[...]))
    step_rows[...] = step * live[:, :heads]
    decay_rows[...] = decay * live[:, :heads]
    spread = jnp.where(
        lax.broadcasted_iota(jnp.int32, (heads, inner), 1) // hdim
        == lax.broadcasted_iota(jnp.int32, (heads, inner), 0), 1.0, 0.0
    ).astype(f32)

    def widen(v):
        return jnp.dot(v, spread, precision=lax.Precision.HIGHEST, preferred_element_type=f32)

    x = x_ref[...]
    b = b_ref[...]
    c = c_ref[...]

    def slot(r, total):
        pltpu.make_async_copy(cache_ref.at[r], states.at[r], in_sem.at[r]).wait()
        here = row_id[:, :nstate] == r
        b_row = jnp.where(here, b.astype(f32), 0.0).astype(jnp.bfloat16)
        c_row = jnp.where(here, c.astype(f32), 0.0).astype(jnp.bfloat16)
        state = states[r]
        flat = state.reshape(inner, nstate)
        total = total + lax.dot_general(
            c_row, flat, (((1,), (1,)), ((), ())), preferred_element_type=f32
        )
        outer = lax.dot_general(x, b_row, (((0,), (0,)), ((), ())), preferred_element_type=f32)
        step_row = step_rows[pl.ds(r, 1), :]
        decay_row = decay_rows[pl.ds(r, 1), :]
        for h in range(heads):
            fresh[r, h] = (
                state[h].astype(f32) * decay_row[:, h : h + 1]
                + outer[h * hdim : (h + 1) * hdim] * step_row[:, h : h + 1]
            ).astype(fresh.dtype)
        pltpu.make_async_copy(fresh.at[r], new_ref.at[r], out_sem.at[r]).start()
        return total

    held = lax.fori_loop(0, slots, slot, jnp.zeros((slots, inner), f32))
    inputs = x.astype(f32)
    mix = jnp.sum(b.astype(f32) * c.astype(f32), axis=1, keepdims=True)
    ys = widen(decay) * held + widen(step) * inputs * mix + widen(skip_ref[...]) * inputs
    gated = ys * jax.nn.silu(z_ref[...].astype(f32))
    scale = lax.rsqrt(jnp.mean(gated * gated, axis=1, keepdims=True) + 1e-05)
    normed = jnp.where(live[:, :1] > 0.5, gated * scale * gain_ref[...], 0.0).astype(jnp.bfloat16)
    weights.wait()
    width = mixed_ref.shape[1]
    tile = 512
    while width % tile:
        tile //= 2

    def columns(k, carry):
        part = pl.ds(pl.multiple_of(k * tile, tile), tile)
        mixed_ref[:, part] = jnp.dot(
            normed, weight[:, part], preferred_element_type=f32
        ).astype(mixed_ref.dtype)
        return carry

    lax.fori_loop(0, width // tile, columns, 0)

    def flush(r, carry):
        pltpu.make_async_copy(fresh.at[r], new_ref.at[r], out_sem.at[r]).wait()
        return carry

    lax.fori_loop(0, slots, flush, 0)


def advance(
    info, active, cache_state, moved, out_weight, x_in, z_in, b_in, c_in, dt_in, dt_bias, a_log,
    d_skip, norm_gain,
):
    slots, heads, hdim, nstate = cache_state.shape
    vmem = pl.BlockSpec(memory_space=pltpu.VMEM)
    smem = pl.BlockSpec(memory_space=pltpu.SMEM)
    hbm = pl.BlockSpec(memory_space=pl.ANY)
    dma = pltpu.SemaphoreType.DMA
    return pl.pallas_call(
        step_kernel,
        out_shape=(
            jax.ShapeDtypeStruct((slots, out_weight.shape[1]), jnp.bfloat16),
            jax.ShapeDtypeStruct(cache_state.shape, jnp.bfloat16),
        ),
        in_specs=[smem, smem, hbm, hbm, hbm] + [vmem] * 9,
        out_specs=(vmem, hbm),
        scratch_shapes=[
            pltpu.VMEM(cache_state.shape, cache_state.dtype),
            pltpu.VMEM(cache_state.shape, jnp.bfloat16),
            pltpu.VMEM(out_weight.shape, out_weight.dtype),
            pltpu.VMEM((slots, heads), jnp.float32),
            pltpu.VMEM((slots, heads), jnp.float32),
            dma((slots,)),
            dma((slots,)),
            dma,
        ],
        compiler_params=pltpu.CompilerParams(vmem_limit_bytes=32 * 1024 * 1024),
        name="decode_step",
    )(
        info, active, cache_state, moved, out_weight, x_in, z_in, b_in, c_in, dt_in,
        dt_bias[None, :], a_log[None, :], d_skip[None, :], norm_gain[None, :],
    )


def body(
    n, cache_state, prefill_state, x_in, z_in, b_in, c_in, dt_in, dt_bias, a_log, d_skip,
    norm_gain, out_weight, active, prefill_count, dest_owner, dest_slot,
):
    rows = prefill_state.shape[0]
    valid = jnp.arange(rows, dtype=jnp.int32) < prefill_count[0]
    owner = jnp.where(valid, dest_owner, -1)
    if n % 4 == 0 and n * prefill_state.size * 2 <= ROOM:
        meta = jnp.concatenate([owner, dest_slot, jnp.zeros((128 - 2 * rows,), jnp.int32)])[None, :]
        moved, info = gather_rows(meta, prefill_state, n)
    else:
        myself = lax.axis_index("batch")
        owners = lax.all_gather(owner, "batch", axis=0)
        places = lax.all_gather(dest_slot, "batch", axis=0)
        states = lax.all_gather(prefill_state, "batch", axis=0)
        hit = owners == myself
        source = jnp.argmax(hit, axis=0)
        column = jnp.arange(rows)
        info = jnp.where(jnp.any(hit, axis=0), places[source, column], -1)
        moved = states[source, column]
    return advance(
        info, active, cache_state, moved, out_weight, x_in, z_in, b_in, c_in, dt_in, dt_bias,
        a_log, d_skip, norm_gain,
    )


def solution(mesh):
    split = ("replica", "batch")
    state, matrix, vector = P(split, None, None, None), P(split, None), P(split)
    in_specs = (state, state) + (matrix,) * 5 + (P(),) * 5 + (vector,) * 4
    return jax.shard_map(
        functools.partial(body, mesh.shape["batch"]), mesh=mesh, in_specs=in_specs,
        out_specs=(matrix, state), check_vma=False,
    )
```

```python
import functools

import jax
import jax.numpy as jnp
from jax import lax
from jax.experimental import pallas as pl
from jax.experimental.pallas import tpu as pltpu
from jax.sharding import PartitionSpec as P

MESH = pl.DeviceIdType.MESH
VMEM_ALL = 67043328
ROOM = 24 * 1024 * 1024


def gather_kernel(
    n, meta_ref, pre_ref, moved_ref, info_ref, buf, meta_buf, meta_smem,
    recv_sem, left_sem, right_sem, across_sem, mate_sem, local_sem,
):
    depth = n // 4
    rows = pre_ref.shape[0]
    me = lax.axis_index("batch")
    z, y, c = me // 4, (me // 2) % 2, me % 2

    def index(zz, yy, cc):
        return (zz * 2 + yy) * 2 + cc

    left, right = index(z - 1, y, c), index(z + 1, y, c)
    across, mate = index(z, 1 - y, c), index(z, y, 1 - c)
    has_left, has_right = z > 0, z < depth - 1

    own_rows = pltpu.make_async_copy(pre_ref, buf.at[me], local_sem.at[1])
    own_rows.start()
    barrier = pltpu.get_barrier_semaphore()

    def greet(other):
        pl.semaphore_signal(barrier, inc=1, device_id={"batch": other}, device_id_type=MESH)

    greet(across)
    greet(mate)
    pl.when(has_left)(lambda: greet(left))
    pl.when(has_right)(lambda: greet(right))
    pl.semaphore_wait(barrier, 2 + has_left.astype(jnp.int32) + has_right.astype(jnp.int32))

    def slot(o, j):
        return meta_buf.at[o] if j == rows else buf.at[o, j]

    def mine(j):
        return meta_ref if j == rows else buf.at[me, j]

    own_rows.wait()

    sent = []

    def send(cond, src, o, j, sem, target):
        copy = pltpu.make_async_remote_copy(
            src_ref=src, dst_ref=slot(o, j), send_sem=sem, recv_sem=recv_sem.at[o, j],
            device_id={"batch": target}, device_id_type=MESH,
        )
        if cond is None:
            copy.start()
        else:
            pl.when(cond)(copy.start)
        sent.append((cond, copy))

    def arrive(o, j):
        pltpu.make_async_remote_copy(
            src_ref=slot(o, j), dst_ref=slot(o, j), send_sem=local_sem.at[0],
            recv_sem=recv_sem.at[o, j], device_id={"batch": mate}, device_id_type=MESH,
        ).wait_recv()

    def both(*conds):
        return functools.reduce(jnp.logical_and, conds)

    order = (rows,) + tuple(range(rows))
    last = rows - 1
    for j in order:
        send(has_left, mine(j), me, j, left_sem.at[z, j], left)
        send(has_right, mine(j), me, j, right_sem.at[z, j], right)
    for j in (rows,) + tuple(reversed(range(rows))):
        send(None, mine(j), me, j, across_sem.at[z, j], across)
    for j in order:
        send(None, mine(j), me, j, mate_sem.at[z * 2 + y, j], mate)
    own_meta = pltpu.make_async_copy(meta_ref, meta_buf.at[me], local_sem.at[2])
    own_meta.start()

    def from_across(t):
        for sign in (1, -1) if t else (1,):
            zz = z + t * sign
            o = index(zz, 1 - y, c)
            inside = both(zz >= 0, zz < depth) if t else None
            for j in (rows,) + tuple(reversed(range(rows))):
                cond = inside
                if t and j == last:
                    cond = both(inside, zz > 0, zz < depth - 1)
                if cond is None:
                    arrive(o, j)
                else:
                    pl.when(cond)(functools.partial(arrive, o, j))
                if not t and j == last:
                    send(both(z == depth - 1, has_left), slot(o, j), o, j, left_sem.at[depth, j], left)
                    send(both(z == 0, has_right), slot(o, j), o, j, right_sem.at[depth, j], right)
                send(cond, slot(o, j), o, j, mate_sem.at[zz * 2 + 1 - y, j], mate)

    def far_end(zz, here, ahead, sem, target):
        o = index(zz, 1 - y, c)
        pl.when(here)(functools.partial(arrive, o, last))
        send(both(here, ahead), slot(o, last), o, last, sem.at[depth, last], target)
        send(here, slot(o, last), o, last, mate_sem.at[zz * 2 + 1 - y, last], mate)

    for s in range(1, depth + 1):
        if s > 1:
            far_end(depth - 1, z == depth - s, has_left, left_sem, left)
            far_end(0, z == s - 1, has_right, right_sem, right)
        if s < depth:
            for j in order:
                for sign in (1, -1):
                    zz = z + s * sign
                    o = index(zz, y, c)
                    inside = both(zz >= 0, zz < depth)
                    pl.when(inside)(functools.partial(arrive, o, j))
                    if sign == 1:
                        send(both(inside, has_left), slot(o, j), o, j, left_sem.at[zz, j], left)
                    else:
                        send(both(inside, has_right), slot(o, j), o, j, right_sem.at[zz, j], right)
                    cond = both(inside, zz > 0, zz < depth - 1) if j == last else inside
                    send(cond, slot(o, j), o, j, across_sem.at[zz, j], across)
                    send(inside, slot(o, j), o, j, mate_sem.at[zz * 2 + y, j], mate)
        from_across(s - 1)
    own_meta.wait()

    def of_mate(j):
        def one(k, carry):
            arrive(k * 2 + 1 - c, j)
            return carry
        lax.fori_loop(0, 2 * depth, one, 0)

    of_mate(rows)
    numbers = pltpu.make_async_copy(meta_buf, meta_smem, local_sem.at[3])
    numbers.start()
    numbers.wait()

    picks = []
    for j in range(rows):
        def look(d, carry, j=j):
            hit = meta_smem[d, 0, j] == me
            source, place = carry
            return jnp.where(hit, d, source), jnp.where(hit, meta_smem[d, 0, rows + j], place)
        source, place = lax.fori_loop(0, n, look, (jnp.int32(0), jnp.int32(-1)))
        picks.append(source)
        info_ref[j] = place
    for j in range(rows):
        of_mate(j)
    for j in range(rows):
        moved_ref[j] = buf[picks[j], j]
    for cond, copy in sent:
        if cond is None:
            copy.wait_send()
        else:
            pl.when(cond)(copy.wait_send)


def gather_rows(meta, prefill_state, n):
    rows = prefill_state.shape[0]
    depth = n // 4
    dma = pltpu.SemaphoreType.DMA
    vmem = pl.BlockSpec(memory_space=pltpu.VMEM)
    smem = pl.BlockSpec(memory_space=pltpu.SMEM)
    hbm = pl.BlockSpec(memory_space=pltpu.HBM)
    return pl.pallas_call(
        functools.partial(gather_kernel, n),
        out_shape=(
            jax.ShapeDtypeStruct(prefill_state.shape, prefill_state.dtype),
            jax.ShapeDtypeStruct((rows,), jnp.int32),
        ),
        in_specs=[vmem, hbm],
        out_specs=(vmem, smem),
        scratch_shapes=[
            pltpu.VMEM((n,) + prefill_state.shape, prefill_state.dtype),
            pltpu.VMEM((n,) + meta.shape, jnp.int32),
            pltpu.SMEM((n,) + meta.shape, jnp.int32),
            dma((n, rows + 1)),
            dma((depth + 1, rows + 1)),
            dma((depth + 1, rows + 1)),
            dma((depth, rows + 1)),
            dma((2 * depth, rows + 1)),
            dma((4,)),
        ],
        compiler_params=pltpu.CompilerParams(
            collective_id=0, has_side_effects=True,
            vmem_limit_bytes=VMEM_ALL,
        ),
        cost_estimate=pl.CostEstimate(
            flops=0, bytes_accessed=16 * n * prefill_state.size * 2, transcendentals=0
        ),
        name="gather_rows",
    )(meta, prefill_state)


def step_kernel(count, *refs):
    given, (mixed_ref, new_ref), held = refs[:count], refs[count : count + 2], refs[count + 2 :]
    (info_ref, active_ref, cache_ref, moved_ref, weight_ref, x_ref, z_ref, b_ref, c_ref, dt_ref,
     bias_ref, log_ref, skip_ref, gain_ref) = held[:count]
    fresh, step_rows, decay_rows, in_sem, out_sem = held[count:]
    loads = [
        pltpu.make_async_copy(source, target, in_sem.at[k])
        for k, (source, target) in enumerate(zip(given, held))
    ]
    weights = loads[4]
    first = loads[:2] + loads[5:]
    for copy in first + loads[2:5]:
        copy.start()
    slots, heads, hdim, nstate = cache_ref.shape
    inner = heads * hdim
    moves = moved_ref.shape[0]
    f32 = jnp.float32

    def is_live(r):
        hit = [info_ref[j] == r for j in range(moves)]
        held = functools.reduce(jnp.logical_or, hit)
        return jnp.where(jnp.logical_or(held, active_ref[r] > 0), 1.0, 0.0).astype(f32)

    for copy in first:
        copy.wait()
    live_scalars = [is_live(r) for r in range(slots)]
    row_id = lax.broadcasted_iota(jnp.int32, (slots, 128), 0)
    live = jnp.zeros((slots, 128), f32)
    for r in range(slots):
        live = jnp.where(row_id == r, live_scalars[r], live)

    step = jax.nn.softplus(dt_ref[...].astype(f32) + bias_ref[...])
    decay = jnp.exp(-step * jnp.exp(log_ref[...]))
    step_rows[...] = step * live[:, :heads]
    decay_rows[...] = decay * live[:, :heads]
    spread = jnp.where(
        lax.broadcasted_iota(jnp.int32, (heads, inner), 1) // hdim
        == lax.broadcasted_iota(jnp.int32, (heads, inner), 0), 1.0, 0.0
    ).astype(f32)

    def widen(v):
        return jnp.dot(v, spread, precision=lax.Precision.HIGHEST, preferred_element_type=f32)

    x = x_ref[...]
    b = b_ref[...]
    c = c_ref[...]

    def slot(r, total):
        here = row_id[:, :nstate] == r
        b_row = jnp.where(here, b.astype(f32), 0.0).astype(jnp.bfloat16)
        c_row = jnp.where(here, c.astype(f32), 0.0).astype(jnp.bfloat16)
        state = cache_ref[r]
        for j in range(moves):
            state = jnp.where(info_ref[j] == r, moved_ref[j], state)
        flat = state.reshape(inner, nstate)
        total = total + lax.dot_general(
            c_row, flat, (((1,), (1,)), ((), ())), preferred_element_type=f32
        )
        outer = lax.dot_general(x, b_row, (((0,), (0,)), ((), ())), preferred_element_type=f32)
        step_row = step_rows[pl.ds(r, 1), :]
        decay_row = decay_rows[pl.ds(r, 1), :]
        for h in range(heads):
            fresh[r, h] = (
                state[h].astype(f32) * decay_row[:, h : h + 1]
                + outer[h * hdim : (h + 1) * hdim] * step_row[:, h : h + 1]
            ).astype(fresh.dtype)
        pltpu.make_async_copy(fresh.at[r], new_ref.at[r], out_sem.at[r]).start()
        return total

    for copy in loads[2:4]:
        copy.wait()
    kept = lax.fori_loop(0, slots, slot, jnp.zeros((slots, inner), f32))
    inputs = x.astype(f32)
    mix = jnp.sum(b.astype(f32) * c.astype(f32), axis=1, keepdims=True)
    ys = widen(decay) * kept + widen(step) * inputs * mix + widen(skip_ref[...]) * inputs
    gated = ys * jax.nn.silu(z_ref[...].astype(f32))
    scale = lax.rsqrt(jnp.mean(gated * gated, axis=1, keepdims=True) + 1e-05)
    normed = jnp.where(live[:, :1] > 0.5, gated * scale * gain_ref[...][None, :], 0.0).astype(jnp.bfloat16)
    weights.wait()
    width = mixed_ref.shape[1]
    tile = 512
    while width % tile:
        tile //= 2

    def columns(k, carry):
        part = pl.ds(pl.multiple_of(k * tile, tile), tile)
        mixed_ref[:, part] = jnp.dot(
            normed, weight_ref[:, part], preferred_element_type=f32
        ).astype(mixed_ref.dtype)
        return carry

    lax.fori_loop(0, width // tile, columns, 0)

    def flush(r, carry):
        pltpu.make_async_copy(fresh.at[r], new_ref.at[r], out_sem.at[r]).wait()
        return carry

    lax.fori_loop(0, slots, flush, 0)


def advance(*given):
    active, cache_state, out_weight, dt_in = given[1], given[2], given[4], given[9]
    hbm = pl.BlockSpec(memory_space=pltpu.HBM)
    dma = pltpu.SemaphoreType.DMA
    count = len(given)
    return pl.pallas_call(
        functools.partial(step_kernel, count),
        out_shape=(
            jax.ShapeDtypeStruct((active.shape[0], out_weight.shape[1]), jnp.bfloat16),
            jax.ShapeDtypeStruct(cache_state.shape, jnp.bfloat16),
        ),
        in_specs=[hbm] * count,
        out_specs=(pl.BlockSpec(memory_space=pltpu.VMEM), hbm),
        scratch_shapes=[
            *(pltpu.SMEM(a.shape, a.dtype) for a in given[:2]),
            *(pltpu.VMEM(a.shape, a.dtype) for a in given[2:]),
            pltpu.VMEM(cache_state.shape, jnp.bfloat16),
            pltpu.VMEM(dt_in.shape, jnp.float32),
            pltpu.VMEM(dt_in.shape, jnp.float32),
            dma((count,)),
            dma((active.shape[0],)),
        ],
        compiler_params=pltpu.CompilerParams(vmem_limit_bytes=VMEM_ALL),
        name="decode_step",
    )(*given)


def body(
    n, cache_state, prefill_state, x_in, z_in, b_in, c_in, dt_in, dt_bias, a_log, d_skip,
    norm_gain, out_weight, active, prefill_count, dest_owner, dest_slot,
):
    rows = prefill_state.shape[0]
    ahead = (
        out_weight, x_in, z_in, b_in, c_in, dt_in, dt_bias[None, :],
        a_log[None, :], d_skip[None, :], norm_gain,
    )
    if n % 4 == 0 and n * prefill_state.size * 2 <= ROOM:
        valid = jnp.arange(rows, dtype=jnp.int32) < prefill_count[0]
        owner = jnp.where(valid, dest_owner, -1)
        meta = (jnp.pad(owner, (0, 128 - rows)) + jnp.pad(dest_slot, (rows, 128 - 2 * rows)))[None, :]
        moved, info = gather_rows(meta, prefill_state, n)
    else:
        valid = jnp.arange(rows, dtype=jnp.int32) < prefill_count[0]
        owner = jnp.where(valid, dest_owner, -1)
        myself = lax.axis_index("batch")
        owners = lax.all_gather(owner, "batch", axis=0)
        places = lax.all_gather(dest_slot, "batch", axis=0)
        states = lax.all_gather(prefill_state, "batch", axis=0)
        hit = owners == myself
        source = jnp.argmax(hit, axis=0)
        column = jnp.arange(rows)
        info = jnp.where(jnp.any(hit, axis=0), places[source, column], -1)
        moved = states[source, column]
    return advance(info, active, cache_state, moved, *ahead)


def solution(mesh):
    split = ("replica", "batch")
    state, matrix, vector = P(split, None, None, None), P(split, None), P(split)
    in_specs = (state, state) + (matrix,) * 5 + (P(),) * 5 + (vector,) * 4
    return jax.shard_map(
        functools.partial(body, mesh.shape["batch"]), mesh=mesh, in_specs=in_specs,
        out_specs=(matrix, state), check_vma=False,
    )
```

```python
import functools

import jax
import jax.numpy as jnp
from jax import lax
from jax.experimental import pallas as pl
from jax.experimental.pallas import tpu as pltpu
from jax.sharding import PartitionSpec as P

MESH = pl.DeviceIdType.MESH
VMEM_ALL = 67043328
ROOM = 24 * 1024 * 1024


def gather_kernel(
    n, owner_ref, place_ref, count_ref, pre_ref, moved_ref, info_ref,
    buf, owner_buf, place_buf, count_buf, owner_all, place_all, count_all,
    recv_sem, left_sem, right_sem, across_sem, mate_sem, local_sem,
):
    depth = n // 4
    rows = pre_ref.shape[0]
    me = lax.axis_index("batch")
    z, y, c = me // 4, (me // 2) % 2, me % 2

    def index(zz, yy, cc):
        return (zz * 2 + yy) * 2 + cc

    left, right = index(z - 1, y, c), index(z + 1, y, c)
    across, mate = index(z, 1 - y, c), index(z, y, 1 - c)
    has_left, has_right = z > 0, z < depth - 1

    own = [
        pltpu.make_async_copy(source, target.at[me], local_sem.at[k])
        for k, (source, target) in enumerate((
            (owner_ref, owner_buf), (place_ref, place_buf), (count_ref, count_buf), (pre_ref, buf)
        ))
    ]
    for copy in own:
        copy.start()
    barrier = pltpu.get_barrier_semaphore()

    def greet(other):
        pl.semaphore_signal(barrier, inc=1, device_id={"batch": other}, device_id_type=MESH)

    greet(across)
    greet(mate)
    pl.when(has_left)(lambda: greet(left))
    pl.when(has_right)(lambda: greet(right))
    pl.semaphore_wait(barrier, 2 + has_left.astype(jnp.int32) + has_right.astype(jnp.int32))

    def slot(o, j):
        return buf.at[o, j] if j < rows else (owner_buf, place_buf, count_buf)[j - rows].at[o]

    def mine(j):
        return slot(me, j)

    for copy in own:
        copy.wait()

    sent = []

    def send(cond, src, o, j, sem, target):
        copy = pltpu.make_async_remote_copy(
            src_ref=src, dst_ref=slot(o, j), send_sem=sem, recv_sem=recv_sem.at[o, j],
            device_id={"batch": target}, device_id_type=MESH,
        )
        if cond is None:
            copy.start()
        else:
            pl.when(cond)(copy.start)
        sent.append((cond, copy))

    def arrive(o, j):
        pltpu.make_async_remote_copy(
            src_ref=slot(o, j), dst_ref=slot(o, j), send_sem=local_sem.at[0],
            recv_sem=recv_sem.at[o, j], device_id={"batch": mate}, device_id_type=MESH,
        ).wait_recv()

    def both(*conds):
        return functools.reduce(jnp.logical_and, conds)

    numbers = (rows, rows + 1, rows + 2)
    order = numbers + tuple(range(rows))
    last = rows - 1
    for j in order:
        send(has_left, mine(j), me, j, left_sem.at[z, j], left)
        send(has_right, mine(j), me, j, right_sem.at[z, j], right)
    for j in numbers + tuple(reversed(range(rows))):
        send(None, mine(j), me, j, across_sem.at[z, j], across)
    for j in order:
        send(None, mine(j), me, j, mate_sem.at[z * 2 + y, j], mate)
    def from_across(t):
        for sign in (1, -1) if t else (1,):
            zz = z + t * sign
            o = index(zz, 1 - y, c)
            inside = both(zz >= 0, zz < depth) if t else None
            for j in numbers + tuple(reversed(range(rows))):
                cond = inside
                if t and j == last:
                    cond = both(inside, zz > 0, zz < depth - 1)
                if cond is None:
                    arrive(o, j)
                else:
                    pl.when(cond)(functools.partial(arrive, o, j))
                if not t and j == last:
                    send(both(z == depth - 1, has_left), slot(o, j), o, j, left_sem.at[depth, j], left)
                    send(both(z == 0, has_right), slot(o, j), o, j, right_sem.at[depth, j], right)
                send(cond, slot(o, j), o, j, mate_sem.at[zz * 2 + 1 - y, j], mate)

    def far_end(zz, here, ahead, sem, target):
        o = index(zz, 1 - y, c)
        pl.when(here)(functools.partial(arrive, o, last))
        send(both(here, ahead), slot(o, last), o, last, sem.at[depth, last], target)
        send(here, slot(o, last), o, last, mate_sem.at[zz * 2 + 1 - y, last], mate)

    for s in range(1, depth + 1):
        if s > 1:
            far_end(depth - 1, z == depth - s, has_left, left_sem, left)
            far_end(0, z == s - 1, has_right, right_sem, right)
        if s < depth:
            for j in order:
                for sign in (1, -1):
                    zz = z + s * sign
                    o = index(zz, y, c)
                    inside = both(zz >= 0, zz < depth)
                    pl.when(inside)(functools.partial(arrive, o, j))
                    if sign == 1:
                        send(both(inside, has_left), slot(o, j), o, j, left_sem.at[zz, j], left)
                    else:
                        send(both(inside, has_right), slot(o, j), o, j, right_sem.at[zz, j], right)
                    cond = both(inside, zz > 0, zz < depth - 1) if j == last else inside
                    send(cond, slot(o, j), o, j, across_sem.at[zz, j], across)
                    send(inside, slot(o, j), o, j, mate_sem.at[zz * 2 + y, j], mate)
        from_across(s - 1)

    def of_mate(j):
        def one(k, carry):
            arrive(k * 2 + 1 - c, j)
            return carry
        lax.fori_loop(0, 2 * depth, one, 0)

    for j in numbers:
        of_mate(j)
    reads = [
        pltpu.make_async_copy(source, target, local_sem.at[k])
        for k, (source, target) in enumerate((
            (owner_buf, owner_all), (place_buf, place_all), (count_buf, count_all)
        ))
    ]
    for copy in reads:
        copy.start()
    for copy in reads:
        copy.wait()

    picks = []
    for j in range(rows):
        def look(d, carry, j=j):
            hit = jnp.logical_and(owner_all[d, 0, j] == me, count_all[d, 0, 0] > j)
            source, place = carry
            return jnp.where(hit, d, source), jnp.where(hit, place_all[d, 0, j], place)
        source, place = lax.fori_loop(0, n, look, (jnp.int32(0), jnp.int32(-1)))
        picks.append(source)
        info_ref[j] = place
    for j in range(rows):
        of_mate(j)
    for j in range(rows):
        moved_ref[j] = buf[picks[j], j]
    for cond, copy in sent:
        if cond is None:
            copy.wait_send()
        else:
            pl.when(cond)(copy.wait_send)


def gather_rows(owner, place, live_rows, prefill_state, n):
    rows = prefill_state.shape[0]
    depth = n // 4
    dma = pltpu.SemaphoreType.DMA
    vmem = pl.BlockSpec(memory_space=pltpu.VMEM)
    smem = pl.BlockSpec(memory_space=pltpu.SMEM)
    hbm = pl.BlockSpec(memory_space=pltpu.HBM)
    return pl.pallas_call(
        functools.partial(gather_kernel, n),
        out_shape=(
            jax.ShapeDtypeStruct(prefill_state.shape, prefill_state.dtype),
            jax.ShapeDtypeStruct((rows,), jnp.int32),
        ),
        in_specs=[hbm] * 4,
        out_specs=(vmem, smem),
        scratch_shapes=[
            pltpu.VMEM((n,) + prefill_state.shape, prefill_state.dtype),
            *(pltpu.VMEM((n,) + a.shape, jnp.int32) for a in (owner, place, live_rows)),
            *(pltpu.SMEM((n,) + a.shape, jnp.int32) for a in (owner, place, live_rows)),
            dma((n, rows + 3)),
            dma((depth + 1, rows + 3)),
            dma((depth + 1, rows + 3)),
            dma((depth, rows + 3)),
            dma((2 * depth, rows + 3)),
            dma((4,)),
        ],
        compiler_params=pltpu.CompilerParams(
            collective_id=0, has_side_effects=True,
            vmem_limit_bytes=VMEM_ALL,
        ),
        cost_estimate=pl.CostEstimate(
            flops=0, bytes_accessed=16 * n * prefill_state.size * 2, transcendentals=0
        ),
        name="gather_rows",
    )(owner, place, live_rows, prefill_state)


def step_kernel(count, *refs):
    given, (mixed_ref, new_ref), held = refs[:count], refs[count : count + 2], refs[count + 2 :]
    (info_ref, active_ref, cache_ref, moved_ref, weight_ref, x_ref, z_ref, b_ref, c_ref, dt_ref,
     bias_ref, log_ref, skip_ref, gain_ref) = held[:count]
    fresh, step_rows, decay_rows, in_sem, out_sem = held[count:]
    loads = [
        pltpu.make_async_copy(source, target, in_sem.at[k])
        for k, (source, target) in enumerate(zip(given, held))
    ]
    weights = loads[4]
    first = loads[:2] + loads[5:]
    for copy in first + loads[2:5]:
        copy.start()
    slots, heads, hdim, nstate = cache_ref.shape
    inner = heads * hdim
    moves = moved_ref.shape[0]
    f32 = jnp.float32

    def is_live(r):
        hit = [info_ref[j] == r for j in range(moves)]
        held = functools.reduce(jnp.logical_or, hit)
        return jnp.where(jnp.logical_or(held, active_ref[r] > 0), 1.0, 0.0).astype(f32)

    for copy in first:
        copy.wait()
    live_scalars = [is_live(r) for r in range(slots)]
    row_id = lax.broadcasted_iota(jnp.int32, (slots, 128), 0)
    live = jnp.zeros((slots, 128), f32)
    for r in range(slots):
        live = jnp.where(row_id == r, live_scalars[r], live)

    step = jax.nn.softplus(dt_ref[...].astype(f32) + bias_ref[...])
    decay = jnp.exp(-step * jnp.exp(log_ref[...]))
    step_rows[...] = step * live[:, :heads]
    decay_rows[...] = decay * live[:, :heads]
    spread = jnp.where(
        lax.broadcasted_iota(jnp.int32, (heads, inner), 1) // hdim
        == lax.broadcasted_iota(jnp.int32, (heads, inner), 0), 1.0, 0.0
    ).astype(f32)

    def widen(v):
        return jnp.dot(v, spread, precision=lax.Precision.HIGHEST, preferred_element_type=f32)

    x = x_ref[...]
    b = b_ref[...]
    c = c_ref[...]

    def slot(r, total):
        here = row_id[:, :nstate] == r
        b_row = jnp.where(here, b.astype(f32), 0.0).astype(jnp.bfloat16)
        c_row = jnp.where(here, c.astype(f32), 0.0).astype(jnp.bfloat16)
        state = cache_ref[r]
        for j in range(moves):
            state = jnp.where(info_ref[j] == r, moved_ref[j], state)
        flat = state.reshape(inner, nstate)
        total = total + lax.dot_general(
            c_row, flat, (((1,), (1,)), ((), ())), preferred_element_type=f32
        )
        outer = lax.dot_general(x, b_row, (((0,), (0,)), ((), ())), preferred_element_type=f32)
        step_row = step_rows[pl.ds(r, 1), :]
        decay_row = decay_rows[pl.ds(r, 1), :]
        for h in range(heads):
            fresh[r, h] = (
                state[h].astype(f32) * decay_row[:, h : h + 1]
                + outer[h * hdim : (h + 1) * hdim] * step_row[:, h : h + 1]
            ).astype(fresh.dtype)
        pltpu.make_async_copy(fresh.at[r], new_ref.at[r], out_sem.at[r]).start()
        return total

    for copy in loads[2:4]:
        copy.wait()
    kept = lax.fori_loop(0, slots, slot, jnp.zeros((slots, inner), f32))
    inputs = x.astype(f32)
    mix = jnp.sum(b.astype(f32) * c.astype(f32), axis=1, keepdims=True)
    ys = widen(decay) * kept + widen(step) * inputs * mix + widen(skip_ref[...]) * inputs
    gated = ys * jax.nn.silu(z_ref[...].astype(f32))
    scale = lax.rsqrt(jnp.mean(gated * gated, axis=1, keepdims=True) + 1e-05)
    normed = jnp.where(live[:, :1] > 0.5, gated * scale * gain_ref[...][None, :], 0.0).astype(jnp.bfloat16)
    weights.wait()
    width = mixed_ref.shape[1]
    tile = 512
    while width % tile:
        tile //= 2

    def columns(k, carry):
        part = pl.ds(pl.multiple_of(k * tile, tile), tile)
        mixed_ref[:, part] = jnp.dot(
            normed, weight_ref[:, part], preferred_element_type=f32
        ).astype(mixed_ref.dtype)
        return carry

    lax.fori_loop(0, width // tile, columns, 0)

    def flush(r, carry):
        pltpu.make_async_copy(fresh.at[r], new_ref.at[r], out_sem.at[r]).wait()
        return carry

    lax.fori_loop(0, slots, flush, 0)


def advance(*given):
    active, cache_state, out_weight, dt_in = given[1], given[2], given[4], given[9]
    hbm = pl.BlockSpec(memory_space=pltpu.HBM)
    dma = pltpu.SemaphoreType.DMA
    count = len(given)
    return pl.pallas_call(
        functools.partial(step_kernel, count),
        out_shape=(
            jax.ShapeDtypeStruct((active.shape[0], out_weight.shape[1]), jnp.bfloat16),
            jax.ShapeDtypeStruct(cache_state.shape, jnp.bfloat16),
        ),
        in_specs=[hbm] * count,
        out_specs=(pl.BlockSpec(memory_space=pltpu.VMEM), hbm),
        scratch_shapes=[
            *(pltpu.SMEM(a.shape, a.dtype) for a in given[:2]),
            *(pltpu.VMEM(a.shape, a.dtype) for a in given[2:]),
            pltpu.VMEM(cache_state.shape, jnp.bfloat16),
            pltpu.VMEM(dt_in.shape, jnp.float32),
            pltpu.VMEM(dt_in.shape, jnp.float32),
            dma((count,)),
            dma((active.shape[0],)),
        ],
        compiler_params=pltpu.CompilerParams(vmem_limit_bytes=VMEM_ALL),
        name="decode_step",
    )(*given)


def body(
    n, cache_state, prefill_state, x_in, z_in, b_in, c_in, dt_in, dt_bias, a_log, d_skip,
    norm_gain, out_weight, active, prefill_count, dest_owner, dest_slot,
):
    rows = prefill_state.shape[0]
    ahead = (
        out_weight, x_in, z_in, b_in, c_in, dt_in, dt_bias[None, :],
        a_log[None, :], d_skip[None, :], norm_gain,
    )
    if n % 4 == 0 and n * prefill_state.size * 2 <= ROOM:
        moved, info = gather_rows(
            dest_owner[None, :], dest_slot[None, :], prefill_count[None, :], prefill_state, n
        )
    else:
        valid = jnp.arange(rows, dtype=jnp.int32) < prefill_count[0]
        owner = jnp.where(valid, dest_owner, -1)
        myself = lax.axis_index("batch")
        owners = lax.all_gather(owner, "batch", axis=0)
        places = lax.all_gather(dest_slot, "batch", axis=0)
        states = lax.all_gather(prefill_state, "batch", axis=0)
        hit = owners == myself
        source = jnp.argmax(hit, axis=0)
        column = jnp.arange(rows)
        info = jnp.where(jnp.any(hit, axis=0), places[source, column], -1)
        moved = states[source, column]
    return advance(info, active, cache_state, moved, *ahead)


def solution(mesh):
    split = ("replica", "batch")
    state, matrix, vector = P(split, None, None, None), P(split, None), P(split)
    in_specs = (state, state) + (matrix,) * 5 + (P(),) * 5 + (vector,) * 4
    return jax.shard_map(
        functools.partial(body, mesh.shape["batch"]), mesh=mesh, in_specs=in_specs,
        out_specs=(matrix, state), check_vma=False,
    )
```
